256 devices in a mesh: rep: 8 (over x, core), shard: 32 (over y, z).
Axes of the slice: x: 4, y: 4, z: 8, core: 2. Of those that a mesh axis runs over, the one named last changes fastest.
Arguments:
- grads: float32 [8, 32, 64, 128, 128], P('rep', 'shard'), may hold values from -24 to 24
- counts: int32 [8, 32, 64, 128], P('rep', 'shard'), may hold values from 0 to 5
- block_owner: int32 [8, 32, 64, 1], P('rep', 'shard'), may hold values from 0 to 31; in each aligned block of 64 rows (0 to 63, 64 to 127, ..., all dimensions but the last counted through in order) at most 4 rows name the same one
- block_local: int32 [8, 32, 64], P('rep', 'shard'), may hold values from 0 to 63
Outputs:
- clipped: float32 [2048, 128, 128], P('shard', 'rep')
The draws below stay inside these ranges and needn't reach their ends.
Inputs may be any that keep to these rules, and one draw needn't show every extreme that they name: `block_owner`: among the 64 blocks of one device no owner is named more than 4 times, a bound that some block reaches.
All inputs are finite; a program needn't handle non-finite values.
Results may differ from the reference program's by a relative error of at most 0.0003.
Values sent between devices are 32-bit elements; how exact they have to be, the bound alone decides.
A program may use at most 128 MiB of HBM per device.

```python
import math
import jax
import jax.numpy as jnp
import numpy as np
from jax import lax

D = 128
BR = 128
BLK_SHARD = 64
KB = 64
CAP = 4
N_REP = 8
N_SHARD = 32


def with_ends(result, stream_key, smallest, largest):
    longest = result.shape.index(max(result.shape))
    spots = []
    for shift in (0, 1):
        where = [jax.random.randint(jax.random.fold_in(stream_key, axis), (), 0, length) for axis, length in enumerate(result.shape)]
        where[longest] = (where[longest] + shift) % result.shape[longest]
        spots.append(tuple(where))
    return result.at[spots[0]].set(smallest).at[spots[1]].set(largest)


def block_scale(own_key, shape, shards, least, top_value):
    def one(axis_at, parts):
        draws = jax.random.uniform(jax.random.fold_in(jax.random.fold_in(own_key, 6), axis_at), (parts,), jnp.float32, least / len(shards), top_value / len(shards))
        return jnp.repeat(jnp.exp(draws), shape[axis_at] // parts).reshape((-1,) + (1,) * (len(shape) - axis_at - 1))

    level = one(*shards[0])
    for cut in shards[1:]:
        level = level * one(*cut)
    return level


def rank_table(amount, slope):
    weights = [(1 << 20) // math.isqrt(standing ** slope) + 1 for standing in range(1, amount + 1)]
    spread = 1 + sum(weights) // (1 << 30)
    return np.cumsum(np.array([max(1, weight // spread) for weight in weights]))


def skewed_ids(rng, dims, amount, skew):
    grid = rank_table(amount, skew)
    lot = jax.random.randint(jax.random.fold_in(rng, 1), dims, 0, int(grid[amount - 1]))
    grade = jnp.searchsorted(jnp.asarray(grid, jnp.int32), lot, side="right")
    return jax.random.permutation(jax.random.fold_in(rng, 2), amount)[grade].astype(jnp.int32)


def shared_out(stream_key, own, number, rows, amount, top, bound, skew):
    sequence = jax.random.permutation(stream_key, amount)
    heavy_load, common = portions_of(amount, rows * top, bound, skew, True), portions_of(amount, rows * top, bound, skew, False)
    places = jnp.arange(amount)

    def named(lengths, rotation):
        used = int((lengths > 0).sum())
        fixed = max(1, used // 4)
        shifted = fixed + (places - fixed + rotation * (used - fixed)) % max(1, amount - fixed)
        return jnp.zeros((amount,), jnp.int32).at[sequence[jnp.where(places < fixed, places, shifted)]].set(jnp.asarray(lengths, jnp.int32))

    lengths = jnp.where(number % 4 == 0, named(heavy_load, number // 4), named(common, number - number // 4 - 1))
    mixed = jax.random.permutation(jax.random.fold_in(own, 3), amount)
    source_of, taker = mixed[0:amount // 2 * 2:2], mixed[1:amount // 2 * 2:2]
    slack = jnp.minimum(lengths[source_of] - 1, bound - lengths[taker]) // 2
    slack = jnp.where((source_of == sequence[0]) | (taker == sequence[0]) | (lengths[taker] == 0), 0, jnp.maximum(slack, 0))
    shifted = jax.random.randint(jax.random.fold_in(own, 4), (amount // 2,), 0, 1 << 20) % (slack + 1)
    lengths = lengths.at[source_of].add(-shifted).at[taker].add(shifted)
    items = jnp.searchsorted(jnp.cumsum(lengths), jnp.arange(rows * top), side="right").astype(jnp.int32)
    listing = items.reshape(top, rows).T
    listing = listing[jax.random.permutation(jax.random.fold_in(own, 1), rows)]
    rotation = jax.random.randint(jax.random.fold_in(own, 2), (rows, 1), 0, top)
    return jnp.take_along_axis(listing, (jnp.arange(top)[None, :] + rotation) % top, axis=1)


def portions_of(amount, total, most, lean, full):
    portions = [(1 << 20) // math.isqrt(grade ** lean) + 1 for grade in range(1, amount + 1)]
    largest = most if full else min(most, max(-(-total // amount), total * portions[0] // sum(portions)))
    least = 1 if total - largest >= amount - 1 else 0
    holding, rest = [largest] + [least] * (amount - 1), total - largest - least * (amount - 1)
    while rest > 0:
        free = [i for i in range(1, amount) if holding[i] < largest] or [i for i in range(1, amount) if holding[i] < most]
        mass, left = sum([portions[i] for i in free]), rest
        for i in free:
            addition = min(most - holding[i], max(1, left * portions[i] // mass), rest)
            holding[i] = holding[i] + addition
            rest = rest - addition
    return np.array(holding)


def noise(stream_key, extent, deviation, most, split=(), held_as=jnp.bfloat16):
    result = jax.random.normal(stream_key, extent, jnp.float32) * deviation
    if len(split) > 0:
        result = block_scale(stream_key, extent, split, -0.22, 0.18) * result
    return jnp.clip(result, min=-most, max=most).astype(held_as)


def setup_inputs(seed: int = 0) -> dict:
    arg_keys = jax.random.split(jax.random.key(seed), 5)
    grads = noise(arg_keys[0], (N_REP, N_SHARD, KB, BR, D), 4.0, 24.0, ((0, 8), (1, 32)), jnp.float32)
    counts = with_ends(jax.random.randint(arg_keys[1], (N_REP, N_SHARD, KB, BR), 0, 6), jax.random.fold_in(arg_keys[1], 1), 0, 5).astype(jnp.int32)
    block_owner_keys = jax.random.split(jax.random.fold_in(arg_keys[2], 1), N_REP * N_SHARD * KB // KB)
    block_owner_turns = jax.random.permutation(jax.random.fold_in(arg_keys[2], 3), N_REP * N_SHARD * KB // KB)
    block_owner = jax.vmap(lambda own, number: shared_out(jax.random.fold_in(arg_keys[2], 2), own, number, KB, N_SHARD, 1, CAP, 2))(block_owner_keys, block_owner_turns).reshape((N_REP, N_SHARD, KB, 1))
    block_local = with_ends(skewed_ids(arg_keys[3], (N_REP, N_SHARD, KB), BLK_SHARD, 2), jax.random.fold_in(arg_keys[3], 3), 0, BLK_SHARD - 1).astype(jnp.int32)
    return dict(grads=grads, counts=counts, block_owner=block_owner, block_local=block_local)


def reference(grads, counts, block_owner, block_local):
    total_blocks = BLK_SHARD * N_SHARD
    block_ids = (block_owner[..., 0] * BLK_SHARD + block_local).astype(jnp.int32)

    def add_replica(carry, items):
        sums, totals = carry
        blocks, cnts, ids = items
        blocks = blocks.reshape(-1, BR, D)
        cnts = cnts.reshape(-1, BR)
        ids = ids.reshape(-1)
        masked = jnp.where(cnts[..., None] > 0, blocks, jnp.float32(0.0))
        sums = sums + jax.ops.segment_sum(masked, ids, total_blocks)
        totals = totals + jax.ops.segment_sum(cnts.astype(jnp.float32), ids, total_blocks)
        return ((sums, totals), None)
    start = (jnp.zeros((total_blocks, BR, D), jnp.float32), jnp.zeros((total_blocks, BR), jnp.float32))
    (sums, totals), unused = lax.scan(add_replica, start, (grads, counts, block_ids))
    mean = sums / jnp.maximum(totals, jnp.float32(1.0))[..., None]
    norm2 = jnp.sum(mean * mean)
    limit = jnp.float32(0.2 * math.sqrt(total_blocks * BR * D))
    scale = jnp.minimum(jnp.float32(1.0), limit / jnp.sqrt(norm2 + jnp.float32(1e-06)))
    return mean * scale
```

```python
import math

import jax
import jax.numpy as jnp
from jax import lax
from jax.experimental import pallas as pl
from jax.experimental.pallas import tpu as pltpu
from jax.sharding import Mesh
from jax.sharding import PartitionSpec as P

NX, NC, NY, NZ = 4, 2, 4, 8
NP = NX * NC * NY
KB, BR, D = 64, 128, 128
BLK = 64
NG = BR // NP
K = NP * KB
CH = NY * BLK
PITCH = BR + 8
MESH = pl.DeviceIdType.MESH
REP = ("x", "c")
SHARD = ("y", "z")
LIMIT = 0.2 * math.sqrt(BLK * NY * NZ * BR * D)


def kernel(
    grads, meta, out,
    nat, xs, rv, mrv, kc, kt, oh, rhs, part, tpart, zr, tzr, ym, yrv, nv, n1, n2s, n2,
    lsem, p1s, p1r, msem, mrsem, zs, zrs, ys, yr, nsem,
):
    x, c, y, z = (lax.axis_index(a) for a in ("x", "c", "y", "z"))
    me = (x * NC + c) * NY + y

    def plane(e):
        px = lax.rem(x + e // (NC * NY), NX)
        pc = lax.rem(c + (e // NY) % NC, NC)
        py = lax.rem(y + e % NY, NY)
        return {"x": px, "c": pc, "y": py}, (px * NC + pc) * NY + py

    def zdev(d):
        return {"z": lax.rem(z + d, NZ)}

    def wait_bytes(ref, sem):
        pltpu.make_async_copy(ref, ref, sem).wait()

    def load(b, _):
        pltpu.make_async_copy(
            grads.at[pl.ds(b * BR, BR)], nat.at[pl.ds(pl.multiple_of(b * PITCH, 8), BR)], lsem
        ).start()
        return 0

    lax.fori_loop(0, KB, load, 0)

    barrier = pltpu.get_barrier_semaphore()

    def greet(e, _):
        pl.semaphore_signal(barrier, inc=1, device_id=plane(e)[0], device_id_type=MESH)
        return 0

    lax.fori_loop(1, NP, greet, 0)

    def greet_z(d, _):
        pl.semaphore_signal(barrier, inc=1, device_id=zdev(d), device_id_type=MESH)
        return 0

    lax.fori_loop(1, NZ, greet_z, 0)
    wait_bytes(nat.at[pl.ds(0, KB * BR)], lsem)

    def prep(g):
        def one(q, _):
            xs[g, q] = nat[pl.ds(q * NG + g, KB, stride=PITCH), :]
            return 0

        lax.fori_loop(0, NP, one, 0)
        rv[g, me] = xs[g, me]

    def send_p1(g):
        def one(i, _):
            dev, q = plane(lax.rem(i * 13 + 8 * g, NP))

            @pl.when(q != me)
            def _():
                pltpu.make_async_remote_copy(
                    src_ref=xs.at[g, q], dst_ref=rv.at[g, me], send_sem=p1s.at[g],
                    recv_sem=p1r.at[g], device_id=dev, device_id_type=MESH,
                ).start()

            return 0

        lax.fori_loop(0, NP, one, 0)

    def z_copy(src, dst, i, k, d):
        return pltpu.make_async_remote_copy(
            src_ref=src, dst_ref=dst, send_sem=zs.at[i, d, k], recv_sem=zrs.at[i, d, k],
            device_id=zdev(1 if d == 0 else NZ - 1), device_id_type=MESH,
        )

    def z_refs(p, r, k, d, half):
        t = 4 - k
        lo, n = (d * half, half) if k == 0 else (0, 2 * half)
        return p.at[t if d == 0 else (NZ - t) % NZ, pl.ds(lo, n)], r.at[d, k, pl.ds(lo, n)]

    def z_step(p, r, i, k, half):
        for d in range(2):
            if k > 0:
                src, dst = z_refs(p, r, k - 1, d, half)
                z_copy(src, dst, i, k - 1, d).wait_recv()
                own, _ = z_refs(p, r, k, d, half)
                if k == 1:
                    own = own.at[pl.ds(d * half, half)]
                own[...] += dst[...]
            src, dst = z_refs(p, r, k, d, half)
            z_copy(src, dst, i, k, d).start()

    def z_final(p, r, i, half):
        for d in range(2):
            src, dst = z_refs(p, r, 3, d, half)
            z_copy(src, dst, i, 3, d).wait_recv()
        return p[0] + r[0, 3] + r[1, 3]

    prep(0)
    pl.semaphore_wait(barrier, NP - 1 + NZ - 1)

    def send_meta(e, _):
        dev, q = plane(e)
        pltpu.make_async_remote_copy(
            src_ref=meta.at[q], dst_ref=mrv.at[me], send_sem=msem, recv_sem=mrsem,
            device_id=dev, device_id_type=MESH,
        ).start()
        return 0

    lax.fori_loop(1, NP, send_meta, 0)
    mrv[me] = meta[me]
    send_p1(0)
    for g in range(1, NG):
        prep(g)
        send_p1(g)

    wait_bytes(mrv.at[pl.ds(0, NP - 1)], mrsem)

    def keys(j, _):
        lane = lax.broadcasted_iota(jnp.int32, (8, 128), 1)
        tile = jnp.where(lane < KB, mrv[2 * j], pltpu.roll(mrv[2 * j + 1], KB, 1))
        row = lax.broadcasted_iota(jnp.int32, (8, 128), 0)
        rel = tile - z * CH
        rel = jnp.where(rel < 0, rel + NZ * CH, rel)
        tile = jnp.where(row == 0, rel, tile)
        kc[:, pl.ds(pl.multiple_of(j * 128, 128), 128)] = tile
        wide = jnp.concatenate([tile.astype(jnp.float32)] * 16, axis=0)
        kt[pl.ds(pl.multiple_of(j * 128, 128), 128), :] = wide.T
        return 0

    lax.fori_loop(0, NP // 2, keys, 0)

    def hot(m, _):
        at = pl.multiple_of(m * 32, 32)
        rows = lax.broadcasted_iota(jnp.int32, (32, K), 0) + at
        key = jnp.broadcast_to(kc[0:1, :], (32, K))
        oh[pl.ds(at, 32), :] = jnp.where(rows == key, 1.0, 0.0).astype(jnp.bfloat16)
        return 0

    lax.fori_loop(0, NZ * CH // 32, hot, 0)

    def total(t, _):
        tot = lax.dot_general(
            kc[...].astype(jnp.float32).astype(jnp.bfloat16), oh[pl.ds(pl.multiple_of(t * CH, CH), CH), :],
            (((1,), (1,)), ((), ())), preferred_element_type=jnp.float32,
        )
        tpart[t, 0:8] = tot[:, 0:128]
        tpart[t, 8:16] = tot[:, 128:256]
        return 0

    lax.fori_loop(0, NZ, total, 0)
    for k in range(4):
        z_step(tpart, tzr, NG, k, 8)
    tots = z_final(tpart, tzr, NG, 8)
    tpart[0] = 1.0 / jnp.maximum(tots, 1.0)

    def combine(g):
        wait_bytes(rv.at[g, pl.ds(0, NP - 1)], p1r.at[g])

        def split(j, _):
            at = pl.ds(pl.multiple_of(j * 128, 128), 128)
            v = rv[g, pl.ds(2 * j, 2)].reshape(128, D)
            v = jnp.where(kt[at, 1 + g : 2 + g] > 0.0, v, 0.0)
            hi = v.astype(jnp.bfloat16)
            rhs[at, 0:D] = hi
            rhs[at, D : 2 * D] = (v - hi.astype(jnp.float32)).astype(jnp.bfloat16)
            return 0

        lax.fori_loop(0, NP // 2, split, 0)

        def chunk(t, _):
            both = jnp.dot(
                oh[pl.ds(pl.multiple_of(t * CH, CH), CH), :], rhs[...],
                preferred_element_type=jnp.float32,
            )
            part[g, t] = both[:, 0:D] + both[:, D : 2 * D]
            return 0

        lax.fori_loop(0, NZ, chunk, 0)

    def finish(g):
        fin = z_final(part.at[g], zr.at[g], g, CH // 2)
        sq = jnp.zeros((8, D), jnp.float32)
        for h in range(2):
            inv = jnp.broadcast_to(tpart[0, 8 * h + 1 + g : 8 * h + 2 + g], (128, 128)).T
            mean = fin[128 * h : 128 * h + 128] * inv
            ym[g, 128 * h : 128 * h + 128] = mean
            sq = sq + jnp.sum((mean * mean).reshape(16, 8, D), axis=0)
        nv[...] = sq if g == 0 else nv[...] + sq

    def send_y(g):
        yrv[g, y] = ym[g, pl.ds(pl.multiple_of(y * BLK, BLK), BLK)]
        for dy in range(1, NY):
            py = lax.rem(y + dy, NY)
            pltpu.make_async_remote_copy(
                src_ref=ym.at[g, pl.ds(pl.multiple_of(py * BLK, BLK), BLK)], dst_ref=yrv.at[g, y],
                send_sem=ys.at[g], recv_sem=yr.at[g], device_id={"y": py}, device_id_type=MESH,
            ).start()

    def step(g, k):
        z_step(part.at[g], zr.at[g], g, k, CH // 2)

    for g in range(NG):
        combine(g)
        step(g, 0)
        if g > 0:
            step(g - 1, 3)
        step(g, 1)
        if g > 0:
            finish(g - 1)
            send_y(g - 1)
        step(g, 2)
    step(NG - 1, 3)
    finish(NG - 1)

    n1[me] = nv[...]

    def norm_plane(e, _):
        dev, _ = plane(e)
        pltpu.make_async_remote_copy(
            src_ref=nv, dst_ref=n1.at[me], send_sem=nsem.at[0], recv_sem=nsem.at[1],
            device_id=dev, device_id_type=MESH,
        ).start()
        return 0

    lax.fori_loop(1, NP, norm_plane, 0)
    send_y(NG - 1)
    wait_bytes(n1.at[pl.ds(0, NP - 1)], nsem.at[1])
    n2s[...] = jnp.sum(n1[...], axis=0)
    n2[z] = n2s[...]

    def norm_z(d, _):
        pltpu.make_async_remote_copy(
            src_ref=n2s, dst_ref=n2.at[z], send_sem=nsem.at[2],
            recv_sem=nsem.at[3], device_id=zdev(d), device_id_type=MESH,
        ).start()
        return 0

    lax.fori_loop(1, NZ, norm_z, 0)
    for g in range(NG):
        wait_bytes(yrv.at[g, pl.ds(0, NY - 1)], yr.at[g])
    wait_bytes(n2.at[pl.ds(0, NZ - 1)], nsem.at[3])
    norm2 = jnp.sum(jnp.sum(n2[...], axis=0), axis=(0, 1), keepdims=True)
    scale = jnp.minimum(1.0, LIMIT / jnp.sqrt(norm2 + 1e-06))
    for g in range(NG):
        for s in range(NY):
            out[pl.ds(s * NG + g, BLK, stride=NY * NG), :] = yrv[g, s] * scale

    wait_bytes(mrv.at[pl.ds(0, NP - 1)], msem)
    for g in range(NG):
        wait_bytes(xs.at[g, pl.ds(0, NP - 1)], p1s.at[g])
        wait_bytes(yrv.at[g, pl.ds(0, NY - 1)], ys.at[g])
    for i in range(NG + 1):
        for k in range(4):
            for d in range(2):
                p, r, half = (tpart, tzr, 8) if i == NG else (part.at[i], zr.at[i], CH // 2)
                z_copy(*z_refs(p, r, k, d, half), i, k, d).wait_send()
    wait_bytes(n1.at[pl.ds(0, NP - 1)], nsem.at[0])
    wait_bytes(n2.at[pl.ds(0, NZ - 1)], nsem.at[2])


def local(grads, counts, block_owner, block_local):
    owner = block_owner.reshape(KB)
    keys = (owner % NZ) * CH + (owner // NZ) * BLK + block_local.reshape(KB)
    rows = counts.reshape(KB, BR).T.reshape(NP, NG, KB)
    meta = jnp.concatenate(
        [jnp.broadcast_to(keys[None, None], (NP, 1, KB)), rows, jnp.zeros((NP, 7 - NG, KB), jnp.int32)],
        axis=1,
    )
    meta = jnp.pad(meta, ((0, 0), (0, 0), (0, 128 - KB)))
    f32 = jnp.float32
    vmem = pltpu.VMEM
    dma = pltpu.SemaphoreType.DMA
    out = pl.pallas_call(
        kernel,
        out_shape=jax.ShapeDtypeStruct((BLK * NY * NG, D), f32),
        in_specs=[pl.BlockSpec(memory_space=pl.ANY), pl.BlockSpec(memory_space=vmem)],
        out_specs=pl.BlockSpec(memory_space=vmem),
        scratch_shapes=[
            vmem((KB * PITCH, D), f32),
            vmem((NG, NP, KB, D), f32),
            vmem((NG, NP, KB, D), f32),
            vmem((NP, 8, 128), jnp.int32),
            vmem((8, K), jnp.int32),
            vmem((K, 128), f32),
            vmem((NZ * CH, K), jnp.bfloat16),
            vmem((K, 2 * D), jnp.bfloat16),
            vmem((NG, NZ, CH, D), f32),
            vmem((NZ, 16, 128), f32),
            vmem((NG, 2, 4, CH, D), f32),
            vmem((2, 4, 16, 128), f32),
            vmem((NG, CH, D), f32),
            vmem((NG, NY, BLK, D), f32),
            vmem((8, D), f32),
            vmem((NP, 8, D), f32),
            vmem((8, D), f32),
            vmem((NZ, 8, D), f32),
            dma,
            dma((NG,)),
            dma((NG,)),
            dma,
            dma,
            dma((NG + 1, 2, 4)),
            dma((NG + 1, 2, 4)),
            dma((NG,)),
            dma((NG,)),
            dma((4,)),
        ],
        compiler_params=pltpu.CompilerParams(
            collective_id=0, has_side_effects=True, vmem_limit_bytes=60 * 2**20
        ),
        name="table_mean",
    )(grads.reshape(KB * BR, D), meta)
    return out.reshape(BLK, NY * NG, D)


def solution(mesh):
    finer = Mesh(mesh.devices.reshape(NX, NC, NY, NZ), ("x", "c", "y", "z"))
    return jax.shard_map(
        local,
        mesh=finer,
        in_specs=(
            P(REP, SHARD, None, None, None),
            P(REP, SHARD, None, None),
            P(REP, SHARD, None, None),
            P(REP, SHARD, None),
        ),
        out_specs=P(SHARD, REP, None),
        check_vma=False,
    )
```

```python
import math

import jax
import jax.numpy as jnp
from jax import lax
from jax.experimental import pallas as pl
from jax.experimental.pallas import tpu as pltpu
from jax.sharding import Mesh
from jax.sharding import PartitionSpec as P

NX, NC, NY, NZ = 4, 2, 4, 8
NP = NX * NC * NY
KB, BR, D = 64, 128, 128
BLK = 64
NG = BR // NP
K = NP * KB
CH = NY * BLK
PITCH = BR + 8
POS = (7, 5, 3, 1, 0, 2, 4, 6)
FIRST = 3
MESH = pl.DeviceIdType.MESH
REP = ("x", "c")
SHARD = ("y", "z")
LIMIT = 0.2 * math.sqrt(BLK * NY * NZ * BR * D)


def kernel(
    grads, counts, owner, ids, out,
    nat, cv, ov, iv, meta, xs, rv, mrv, kc, kt, oh, rhs, part, tpart, zr, tzr, ym, yrv, nv, n1, n2s, n2,
    lsem, csem, p1s, p1r, msem, mrsem, zs, zrs, ys, yr, nsem,
):
    x, c, y, z = (lax.axis_index(a) for a in ("x", "c", "y", "z"))
    me = (x * NC + c) * NY + y
    px = [lax.rem(x + d, NX) for d in range(NX)]
    pc = [c, 1 - c]
    py = [lax.rem(y + d, NY) for d in range(NY)]

    def plane(e):
        dx, dc, dy = e // (NC * NY), (e // NY) % NC, e % NY
        return {"x": px[dx], "c": pc[dc], "y": py[dy]}, (px[dx] * NC + pc[dc]) * NY + py[dy]

    def zdev(d):
        return {"z": lax.rem(z + d, NZ)}

    def wait_bytes(ref, sem):
        pltpu.make_async_copy(ref, ref, sem).wait()

    small = [
        pltpu.make_async_copy(s, d, csem.at[i])
        for i, (s, d) in enumerate(((counts, cv), (owner, ov), (ids, iv)))
    ]
    for cp in small:
        cp.start()

    def load(b, _):
        pltpu.make_async_copy(
            grads.at[pl.ds(pl.multiple_of(b * BR, 8), BR)],
            nat.at[pl.ds(pl.multiple_of(b * PITCH, 8), BR)], lsem,
        ).start()
        return 0

    barrier = pltpu.get_barrier_semaphore()
    for e in range(1, NP):
        pl.semaphore_signal(barrier, inc=1, device_id=plane(e)[0], device_id_type=MESH)
    for d in range(1, NZ):
        pl.semaphore_signal(barrier, inc=1, device_id=zdev(d), device_id_type=MESH)
    lax.fori_loop(0, KB, load, 0, unroll=8)

    for cp in small:
        cp.wait()
    o = ov[...]
    key = ((o & (NZ - 1)) * CH + (o >> 3) * BLK + iv[...]).astype(jnp.float32)
    key = jnp.broadcast_to(jnp.concatenate([key, key], axis=1), (8, 128))
    cf = cv[...].astype(jnp.float32)
    ct = jnp.concatenate([cf, cf], axis=0).T
    low = lax.broadcasted_iota(jnp.int32, (8, 128), 0) < NG
    for j in range(NP // 2):
        two = ct[8 * j : 8 * j + 8]
        meta[2 * j] = jnp.where(low, two, key)
        meta[2 * j + 1] = jnp.where(low, pltpu.roll(two, NG, 0), key)

    def prep(g):
        def one(q, _):
            xs[g, q] = nat[pl.ds(q * NG + g, KB, stride=PITCH), :]
            return 0

        lax.fori_loop(0, NP, one, 0, unroll=4)
        rv[g, me] = xs[g, me]

    def send_plane(e, src, dst, send, recv):
        dev, q = plane(e)
        pltpu.make_async_remote_copy(
            src_ref=src.at[q] if src is not nv else src, dst_ref=dst.at[me], send_sem=send, recv_sem=recv,
            device_id=dev, device_id_type=MESH,
        ).start()

    def send_p1(g):
        for i in range(NP):
            e = (i * 13 + 8 * g) % NP
            if e:
                send_plane(e, xs.at[g], rv.at[g], p1s.at[g], p1r.at[g])

    def z_copy(src, dst, i, k, d, u):
        return pltpu.make_async_remote_copy(
            src_ref=src, dst_ref=dst, send_sem=zs.at[i, d, u, k], recv_sem=zrs.at[i, d, u, k],
            device_id=zdev(1 if d == 0 else NZ - 1), device_id_type=MESH,
        )

    def z_refs(p, r, k, d, u, half):
        t = 4 - k if d == 0 else 4 + k
        return p.at[POS[t % NZ], pl.ds(u * half, half)], r.at[d, u, k]

    def z_step(p, r, i, j, half):
        for far in (1, 0):
            for d in range(2):
                u = d if far else 1 - d
                k = j if far else j + 1
                if k > 3:
                    continue
                own, slot = z_refs(p, r, k, d, u, half)
                if j > 0:
                    src, dst = z_refs(p, r, k - 1, d, u, half)
                    z_copy(src, dst, i, k - 1, d, u).wait_recv()
                    own[...] += dst[...]
                z_copy(own, slot, i, k, d, u).start()

    def z_final(p, r, i, u, half):
        for d in range(2):
            src, dst = z_refs(p, r, 3, d, u, half)
            z_copy(src, dst, i, 3, d, u).wait_recv()
        return p[POS[0], u * half : u * half + half] + r[0, u, 3] + r[1, u, 3]

    pl.semaphore_wait(barrier, NP - 1 + NZ - 1)
    for e in range(1, NP):
        send_plane(e, meta, mrv, msem, mrsem)
    mrv[me] = meta[me]
    wait_bytes(nat.at[pl.ds(0, KB * BR)], lsem)
    for g in range(NG):
        prep(g)
        send_p1(g)

    wait_bytes(mrv.at[pl.ds(0, NP - 1)], mrsem)

    def keys(j, _):
        lane = lax.broadcasted_iota(jnp.int32, (8, 128), 1)
        tile = jnp.where(lane < KB, mrv[2 * j], mrv[2 * j + 1])
        row = lax.broadcasted_iota(jnp.int32, (8, 128), 0)
        at = tile.astype(jnp.int32)
        t = (at >> 8) - z
        t = jnp.where(t < 0, t + NZ, t)
        t = jnp.where(t < 4, 7 - 2 * t, 2 * t - 8)
        tile = jnp.where(row < NG, tile, (t * CH + (at & (CH - 1))).astype(jnp.float32))
        kc[:, pl.ds(pl.multiple_of(j * 128, 128), 128)] = tile
        wide = jnp.concatenate([tile] * 16, axis=0)
        kt[pl.ds(pl.multiple_of(j * 128, 128), 128), :] = wide.T
        return 0

    lax.fori_loop(0, NP // 2, keys, 0, unroll=2)

    def hot(m, _):
        at = pl.multiple_of(m * 32, 32)
        rows = lax.broadcasted_iota(jnp.int32, (32, K), 0) + at
        key = jnp.broadcast_to(kc[NG : NG + 1, :].astype(jnp.int32), (32, K))
        oh[pl.ds(at, 32), :] = jnp.where(rows == key, 1.0, 0.0).astype(jnp.bfloat16)
        return 0

    lax.fori_loop(0, NZ * CH // 32, hot, 0)

    def total(t, _):
        tot = lax.dot_general(
            kc[...].astype(jnp.bfloat16), oh[pl.ds(pl.multiple_of(t * CH, CH), CH), :],
            (((1,), (1,)), ((), ())), preferred_element_type=jnp.float32,
        )
        tpart[t, 0:8] = tot[:, 0:128]
        tpart[t, 8:16] = tot[:, 128:256]
        return 0

    lax.fori_loop(0, NZ, total, 0)

    def split(g):
        wait_bytes(rv.at[g, pl.ds(0, NP - 1)], p1r.at[g])

        def one(j, _):
            at = pl.ds(pl.multiple_of(j * 128, 128), 128)
            v = rv[g, pl.ds(2 * j, 2)].reshape(128, D)
            v = jnp.where(kt[at, g : g + 1] > 0.0, v, 0.0)
            hi = v.astype(jnp.bfloat16)
            rhs[at, 0:D] = hi
            rhs[at, D : 2 * D] = (v - hi.astype(jnp.float32)).astype(jnp.bfloat16)
            return 0

        lax.fori_loop(0, NP // 2, one, 0, unroll=4)

    def combine(g, lo, n):
        both = jnp.dot(oh[lo * CH : (lo + n) * CH, :], rhs[...], preferred_element_type=jnp.float32)
        part[g, lo : lo + n] = (both[:, 0:D] + both[:, D : 2 * D]).reshape(n, CH, D)

    def finish(g):
        sq = jnp.zeros((8, D), jnp.float32)
        for h in range(2):
            fin = z_final(part.at[g], zr.at[g], g, h, CH // 2)
            inv = jnp.broadcast_to(tpart[POS[0], 8 * h + g : 8 * h + g + 1], (128, 128)).T
            mean = fin * inv
            ym[g, 128 * h : 128 * h + 128] = mean
            sq = sq + jnp.sum((mean * mean).reshape(16, 8, D), axis=0)
        nv[...] = sq if g == 0 else nv[...] + sq

    def send_y(g):
        yrv[g, y] = ym[g, pl.ds(pl.multiple_of(y * BLK, BLK), BLK)]
        for dy in range(1, NY):
            pltpu.make_async_remote_copy(
                src_ref=ym.at[g, pl.ds(pl.multiple_of(py[dy] * BLK, BLK), BLK)], dst_ref=yrv.at[g, y],
                send_sem=ys.at[g], recv_sem=yr.at[g], device_id={"y": py[dy]}, device_id_type=MESH,
            ).start()

    def step(g, j):
        z_step(part.at[g], zr.at[g], g, j, CH // 2)

    z_step(tpart, tzr, NG, 0, 8)
    for g in range(NG):
        split(g)
        combine(g, 0, FIRST)
        step(g, 0)
        if g == 0:
            z_step(tpart, tzr, NG, 1, 8)
        combine(g, FIRST, NZ - FIRST)
        if g > 0:
            finish(g - 1)
            send_y(g - 1)
        for j in range(1, 4):
            step(g, j)
            if g == 0 and j < 3:
                z_step(tpart, tzr, NG, j + 1, 8)
        if g == 0:
            for u in range(2):
                tots = z_final(tpart, tzr, NG, u, 8)
                tpart[POS[0], 8 * u : 8 * u + 8] = 1.0 / jnp.maximum(tots, 1.0)
    finish(NG - 1)

    for e in range(1, NP):
        send_plane(e, nv, n1, nsem.at[0], nsem.at[1])
    n1[me] = nv[...]
    send_y(NG - 1)
    wait_bytes(n1.at[pl.ds(0, NP - 1)], nsem.at[1])
    n2s[...] = jnp.sum(n1[...], axis=0)
    for d in range(1, NZ):
        pltpu.make_async_remote_copy(
            src_ref=n2s, dst_ref=n2.at[z], send_sem=nsem.at[2], recv_sem=nsem.at[3],
            device_id=zdev(d), device_id_type=MESH,
        ).start()
    n2[z] = n2s[...]
    for g in range(NG):
        wait_bytes(yrv.at[g, pl.ds(0, NY - 1)], yr.at[g])
    wait_bytes(n2.at[pl.ds(0, NZ - 1)], nsem.at[3])
    norm2 = jnp.sum(jnp.sum(n2[...], axis=0), axis=(0, 1), keepdims=True)
    scale = jnp.minimum(1.0, LIMIT / jnp.sqrt(norm2 + 1e-06))
    for g in range(NG):
        for s in range(NY):
            out[pl.ds(s * NG + g, BLK, stride=NY * NG), :] = yrv[g, s] * scale

    wait_bytes(mrv.at[pl.ds(0, NP - 1)], msem)
    for g in range(NG):
        wait_bytes(xs.at[g, pl.ds(0, NP - 1)], p1s.at[g])
        wait_bytes(yrv.at[g, pl.ds(0, NY - 1)], ys.at[g])
    for i in range(NG + 1):
        p, r, half = (tpart, tzr, 8) if i == NG else (part.at[i], zr.at[i], CH // 2)
        for d in range(2):
            for u in range(2):
                for k in range(0 if u == d else 1, 4):
                    z_copy(*z_refs(p, r, k, d, u, half), i, k, d, u).wait_send()
    wait_bytes(n1.at[pl.ds(0, NP - 1)], nsem.at[0])
    wait_bytes(n2.at[pl.ds(0, NZ - 1)], nsem.at[2])


def local(grads, counts, block_owner, block_local):
    f32 = jnp.float32
    i32 = jnp.int32
    vmem = pltpu.VMEM
    dma = pltpu.SemaphoreType.DMA
    out = pl.pallas_call(
        kernel,
        out_shape=jax.ShapeDtypeStruct((BLK * NY * NG, D), f32),
        in_specs=[pl.BlockSpec(memory_space=pl.ANY)] * 4,
        out_specs=pl.BlockSpec(memory_space=vmem),
        scratch_shapes=[
            vmem((KB * PITCH, D), f32),
            vmem((KB, BR), i32),
            vmem((1, KB), i32),
            vmem((1, KB), i32),
            vmem((NP, 8, 128), f32),
            vmem((NG, NP, KB, D), f32),
            vmem((NG, NP, KB, D), f32),
            vmem((NP, 8, 128), f32),
            vmem((8, K), f32),
            vmem((K, 128), f32),
            vmem((NZ * CH, K), jnp.bfloat16),
            vmem((K, 2 * D), jnp.bfloat16),
            vmem((NG, NZ, CH, D), f32),
            vmem((NZ, 16, 128), f32),
            vmem((NG, 2, 2, 4, CH // 2, D), f32),
            vmem((2, 2, 4, 8, 128), f32),
            vmem((NG, CH, D), f32),
            vmem((NG, NY, BLK, D), f32),
            vmem((8, D), f32),
            vmem((NP, 8, D), f32),
            vmem((8, D), f32),
            vmem((NZ, 8, D), f32),
            dma,
            dma((3,)),
            dma((NG,)),
            dma((NG,)),
            dma,
            dma,
            dma((NG + 1, 2, 2, 4)),
            dma((NG + 1, 2, 2, 4)),
            dma((NG,)),
            dma((NG,)),
            dma((4,)),
        ],
        compiler_params=pltpu.CompilerParams(
            collective_id=0, has_side_effects=True, vmem_limit_bytes=60 * 2**20
        ),
        name="table_mean",
    )(
        grads.reshape(KB * BR, D),
        counts.reshape(KB, BR),
        block_owner.reshape(1, KB),
        block_local.reshape(1, KB),
    )
    return out.reshape(BLK, NY * NG, D)


def solution(mesh):
    finer = Mesh(mesh.devices.reshape(NX, NC, NY, NZ), ("x", "c", "y", "z"))
    return jax.shard_map(
        local,
        mesh=finer,
        in_specs=(
            P(REP, SHARD, None, None, None),
            P(REP, SHARD, None, None),
            P(REP, SHARD, None, None),
            P(REP, SHARD, None),
        ),
        out_specs=P(SHARD, REP, None),
        check_vma=False,
    )
```

```python
import math

import jax
import jax.numpy as jnp
from jax import lax
from jax.experimental import pallas as pl
from jax.experimental.pallas import tpu as pltpu
from jax.sharding import Mesh
from jax.sharding import PartitionSpec as P

NX, NC, NY, NZ = 4, 2, 4, 8
NP = NX * NC * NY
KB, BR, D = 64, 128, 128
BLK = 64
NG = BR // NP
K = NP * KB
CH = NY * BLK
PITCH = BR + 8
POS = (7, 5, 3, 1, 0, 2, 4, 6)
FIRST = 3
SUB = 2
MESH = pl.DeviceIdType.MESH
REP = ("x", "c")
SHARD = ("y", "z")
LIMIT = 0.2 * math.sqrt(BLK * NY * NZ * BR * D)


def kernel(
    grads, counts, owner, ids, out,
    nat, cv, ov, iv, meta, xs, rv, mrv, kc, kt, oh, rhs, part, tpart, zr, tzr, ym, yrv, nv, n1, n2s, n2,
    lsem, csem, p1s, p1r, msem, mrsem, zs, zrs, ys, yr, nsem,
):
    x, c, y, z = (lax.axis_index(a) for a in ("x", "c", "y", "z"))
    me = (x * NC + c) * NY + y
    px = [lax.rem(x + d, NX) for d in range(NX)]
    pc = [c, 1 - c]
    py = [lax.rem(y + d, NY) for d in range(NY)]

    def plane(e):
        dx, dc, dy = e // (NC * NY), (e // NY) % NC, e % NY
        return {"x": px[dx], "c": pc[dc], "y": py[dy]}, (px[dx] * NC + pc[dc]) * NY + py[dy]

    def zdev(d):
        return {"z": lax.rem(z + d, NZ)}

    def wait_bytes(ref, sem):
        pltpu.make_async_copy(ref, ref, sem).wait()

    small = [
        pltpu.make_async_copy(s, d, csem.at[i])
        for i, (s, d) in enumerate(((counts, cv), (owner, ov), (ids, iv)))
    ]
    for cp in small:
        cp.start()

    def load(b, _):
        pltpu.make_async_copy(
            grads.at[pl.ds(pl.multiple_of(b * BR, 8), BR)],
            nat.at[pl.ds(pl.multiple_of(b * PITCH, 8), BR)], lsem,
        ).start()
        return 0

    lax.fori_loop(0, KB, load, 0, unroll=8)
    barrier = pltpu.get_barrier_semaphore()
    for e in range(1, NP):
        pl.semaphore_signal(barrier, inc=1, device_id=plane(e)[0], device_id_type=MESH)
    for d in range(1, NZ):
        pl.semaphore_signal(barrier, inc=1, device_id=zdev(d), device_id_type=MESH)

    for cp in small:
        cp.wait()
    o = ov[...]
    key = ((o & (NZ - 1)) * CH + (o >> 3) * BLK + iv[...]).astype(jnp.float32)
    key = jnp.broadcast_to(jnp.concatenate([key, key], axis=1), (8, 128))
    cf = cv[...].astype(jnp.float32)
    ct = jnp.concatenate([cf, cf], axis=0).T
    low = lax.broadcasted_iota(jnp.int32, (8, 128), 0) < NG
    for j in range(NP // 2):
        two = ct[8 * j : 8 * j + 8]
        meta[2 * j] = jnp.where(low, two, key)
        meta[2 * j + 1] = jnp.where(low, pltpu.roll(two, NG, 0), key)

    def prep(g):
        def one(q, _):
            xs[g, q] = nat[pl.ds(q * NG + g, KB, stride=PITCH), :]
            return 0

        lax.fori_loop(0, NP, one, 0, unroll=4)
        rv[g, me] = xs[g, me]

    def send_plane(e, src, dst, send, recv):
        dev, q = plane(e)
        pltpu.make_async_remote_copy(
            src_ref=src.at[q] if src is not nv else src, dst_ref=dst.at[me], send_sem=send, recv_sem=recv,
            device_id=dev, device_id_type=MESH,
        ).start()

    def send_p1(g):
        for i in range(NP):
            e = (i * 13 + 8 * g) % NP
            if e:
                send_plane(e, xs.at[g], rv.at[g], p1s.at[g], p1r.at[g])

    def z_copy(src, dst, i, k, d, u):
        return pltpu.make_async_remote_copy(
            src_ref=src, dst_ref=dst, send_sem=zs.at[i, d, u, k], recv_sem=zrs.at[i, d, u, k],
            device_id=zdev(1 if d == 0 else NZ - 1), device_id_type=MESH,
        )

    def z_refs(p, r, k, d, u, n):
        t = 4 - k if d == 0 else 4 + k
        return p.at[POS[t % NZ], pl.ds(u * n, n)], r.at[d, u, k]

    def far(d, u, n):
        return (u * 2 * n < rows_of(n)) == (d == 0)

    def rows_of(n):
        return 16 if n == 8 else CH

    def z_step(p, r, i, j, n):
        parts = rows_of(n) // n
        for first in (True, False):
            for v in range(parts // 2):
                for d in range(2):
                    u = v if (d == 0) == first else parts // 2 + v
                    k = j if first else j + 1
                    if k > 3:
                        continue
                    own, slot = z_refs(p, r, k, d, u, n)
                    if j > 0:
                        src, dst = z_refs(p, r, k - 1, d, u, n)
                        z_copy(src, dst, i, k - 1, d, u).wait_recv()
                        own[...] += dst[...]
                    z_copy(own, slot, i, k, d, u).start()

    def z_final(p, r, i, u, n):
        for d in range(2):
            src, dst = z_refs(p, r, 3, d, u, n)
            z_copy(src, dst, i, 3, d, u).wait_recv()
        return p[POS[0], u * n : u * n + n] + r[0, u, 3] + r[1, u, 3]

    wait_bytes(nat.at[pl.ds(0, KB * BR)], lsem)
    prep(0)
    pl.semaphore_wait(barrier, NP - 1 + NZ - 1)
    for e in range(1, NP):
        send_plane(e, meta, mrv, msem, mrsem)
    send_p1(0)
    mrv[me] = meta[me]
    for g in range(1, NG):
        prep(g)
        send_p1(g)

    wait_bytes(mrv.at[pl.ds(0, NP - 1)], mrsem)

    def keys(j, _):
        lane = lax.broadcasted_iota(jnp.int32, (8, 128), 1)
        tile = jnp.where(lane < KB, mrv[2 * j], mrv[2 * j + 1])
        row = lax.broadcasted_iota(jnp.int32, (8, 128), 0)
        at = tile.astype(jnp.int32)
        t = (at >> 8) - z
        t = jnp.where(t < 0, t + NZ, t)
        t = jnp.where(t < 4, 7 - 2 * t, 2 * t - 8)
        tile = jnp.where(row < NG, tile, (t * CH + (at & (CH - 1))).astype(jnp.float32))
        kc[:, pl.ds(pl.multiple_of(j * 128, 128), 128)] = tile
        wide = jnp.concatenate([tile] * 16, axis=0)
        kt[pl.ds(pl.multiple_of(j * 128, 128), 128), :] = wide.T
        return 0

    lax.fori_loop(0, NP // 2, keys, 0, unroll=2)

    def hot(m, _):
        at = pl.multiple_of(m * 32, 32)
        rows = lax.broadcasted_iota(jnp.int32, (32, K), 0) + at
        key = jnp.broadcast_to(kc[NG : NG + 1, :].astype(jnp.int32), (32, K))
        oh[pl.ds(at, 32), :] = jnp.where(rows == key, 1.0, 0.0).astype(jnp.bfloat16)
        return 0

    lax.fori_loop(0, NZ * CH // 32, hot, 0)

    def total(t, _):
        tot = lax.dot_general(
            kc[...].astype(jnp.bfloat16), oh[pl.ds(pl.multiple_of(t * CH, CH), CH), :],
            (((1,), (1,)), ((), ())), preferred_element_type=jnp.float32,
        )
        tpart[t, 0:8] = tot[:, 0:128]
        tpart[t, 8:16] = tot[:, 128:256]
        return 0

    lax.fori_loop(0, NZ, total, 0)

    def split(g):
        wait_bytes(rv.at[g, pl.ds(0, NP - 1)], p1r.at[g])

        def one(j, _):
            at = pl.ds(pl.multiple_of(j * 128, 128), 128)
            v = rv[g, pl.ds(2 * j, 2)].reshape(128, D)
            v = jnp.where(kt[at, g : g + 1] > 0.0, v, 0.0)
            hi = v.astype(jnp.bfloat16)
            rhs[at, 0:D] = hi
            rhs[at, D : 2 * D] = (v - hi.astype(jnp.float32)).astype(jnp.bfloat16)
            return 0

        lax.fori_loop(0, NP // 2, one, 0, unroll=4)

    def combine(g, lo, n):
        both = jnp.dot(oh[lo * CH : (lo + n) * CH, :], rhs[...], preferred_element_type=jnp.float32)
        part[g, lo : lo + n] = (both[:, 0:D] + both[:, D : 2 * D]).reshape(n, CH, D)

    def finish(g):
        n = CH // SUB
        sq = jnp.zeros((8, D), jnp.float32)
        inv = [
            jnp.broadcast_to(tpart[POS[0], 8 * h + g : 8 * h + g + 1], (128, 128)).T for h in range(2)
        ]
        for v in range(SUB // 2):
            for u in (v, SUB // 2 + v):
                fin = z_final(part.at[g], zr.at[g], g, u, n)
                mean = fin * inv[u * n // 128][u * n % 128 : u * n % 128 + n]
                ym[g, u * n : u * n + n] = mean
                sq = sq + jnp.sum((mean * mean).reshape(n // 8, 8, D), axis=0)
        nv[...] = sq if g == 0 else nv[...] + sq

    def send_y(g):
        yrv[g, y] = ym[g, pl.ds(pl.multiple_of(y * BLK, BLK), BLK)]
        for dy in range(1, NY):
            pltpu.make_async_remote_copy(
                src_ref=ym.at[g, pl.ds(pl.multiple_of(py[dy] * BLK, BLK), BLK)], dst_ref=yrv.at[g, y],
                send_sem=ys.at[g], recv_sem=yr.at[g], device_id={"y": py[dy]}, device_id_type=MESH,
            ).start()

    def step(g, j):
        z_step(part.at[g], zr.at[g], g, j, CH // SUB)

    z_step(tpart, tzr, NG, 0, 8)
    for g in range(NG):
        split(g)
        combine(g, 0, FIRST)
        step(g, 0)
        if g == 0:
            z_step(tpart, tzr, NG, 1, 8)
        combine(g, FIRST, NZ - FIRST)
        if g > 0:
            step(g - 1, 3)
        step(g, 1)
        if g == 0:
            z_step(tpart, tzr, NG, 2, 8)
        if g == 1:
            for u in range(2):
                tots = z_final(tpart, tzr, NG, u, 8)
                tpart[POS[0], 8 * u : 8 * u + 8] = 1.0 / jnp.maximum(tots, 1.0)
        if g > 0:
            finish(g - 1)
            send_y(g - 1)
        step(g, 2)
        if g == 0:
            z_step(tpart, tzr, NG, 3, 8)
    step(NG - 1, 3)
    finish(NG - 1)

    for e in range(1, NP):
        send_plane(e, nv, n1, nsem.at[0], nsem.at[1])
    n1[me] = nv[...]
    send_y(NG - 1)
    wait_bytes(n1.at[pl.ds(0, NP - 1)], nsem.at[1])
    n2s[...] = jnp.sum(n1[...], axis=0)
    for d in range(1, NZ):
        pltpu.make_async_remote_copy(
            src_ref=n2s, dst_ref=n2.at[z], send_sem=nsem.at[2], recv_sem=nsem.at[3],
            device_id=zdev(d), device_id_type=MESH,
        ).start()
    n2[z] = n2s[...]
    for g in range(NG):
        wait_bytes(yrv.at[g, pl.ds(0, NY - 1)], yr.at[g])
    wait_bytes(n2.at[pl.ds(0, NZ - 1)], nsem.at[3])
    norm2 = jnp.sum(jnp.sum(n2[...], axis=0), axis=(0, 1), keepdims=True)
    scale = jnp.minimum(1.0, LIMIT / jnp.sqrt(norm2 + 1e-06))
    for g in range(NG):
        for s in range(NY):
            out[pl.ds(s * NG + g, BLK, stride=NY * NG), :] = yrv[g, s] * scale

    wait_bytes(mrv.at[pl.ds(0, NP - 1)], msem)
    for g in range(NG):
        wait_bytes(xs.at[g, pl.ds(0, NP - 1)], p1s.at[g])
        wait_bytes(yrv.at[g, pl.ds(0, NY - 1)], ys.at[g])
    for i in range(NG + 1):
        p, r, n = (tpart, tzr, 8) if i == NG else (part.at[i], zr.at[i], CH // SUB)
        for d in range(2):
            for u in range(rows_of(n) // n):
                for k in range(0 if far(d, u, n) else 1, 4):
                    z_copy(*z_refs(p, r, k, d, u, n), i, k, d, u).wait_send()
    wait_bytes(n1.at[pl.ds(0, NP - 1)], nsem.at[0])
    wait_bytes(n2.at[pl.ds(0, NZ - 1)], nsem.at[2])


def local(grads, counts, block_owner, block_local):
    f32 = jnp.float32
    i32 = jnp.int32
    vmem = pltpu.VMEM
    dma = pltpu.SemaphoreType.DMA
    out = pl.pallas_call(
        kernel,
        out_shape=jax.ShapeDtypeStruct((BLK * NY * NG, D), f32),
        in_specs=[pl.BlockSpec(memory_space=pl.ANY)] * 4,
        out_specs=pl.BlockSpec(memory_space=vmem),
        scratch_shapes=[
            vmem((KB * PITCH, D), f32),
            vmem((KB, BR), i32),
            vmem((1, KB), i32),
            vmem((1, KB), i32),
            vmem((NP, 8, 128), f32),
            vmem((NG, NP, KB, D), f32),
            vmem((NG, NP, KB, D), f32),
            vmem((NP, 8, 128), f32),
            vmem((8, K), f32),
            vmem((K, 128), f32),
            vmem((NZ * CH, K), jnp.bfloat16),
            vmem((K, 2 * D), jnp.bfloat16),
            vmem((NG, NZ, CH, D), f32),
            vmem((NZ, 16, 128), f32),
            vmem((NG, 2, SUB, 4, CH // SUB, D), f32),
            vmem((2, 2, 4, 8, 128), f32),
            vmem((NG, CH, D), f32),
            vmem((NG, NY, BLK, D), f32),
            vmem((8, D), f32),
            vmem((NP, 8, D), f32),
            vmem((8, D), f32),
            vmem((NZ, 8, D), f32),
            dma,
            dma((3,)),
            dma((NG,)),
            dma((NG,)),
            dma,
            dma,
            dma((NG + 1, 2, SUB, 4)),
            dma((NG + 1, 2, SUB, 4)),
            dma((NG,)),
            dma((NG,)),
            dma((4,)),
        ],
        compiler_params=pltpu.CompilerParams(
            collective_id=0, has_side_effects=True, vmem_limit_bytes=60 * 2**20
        ),
        name="table_mean",
    )(
        grads.reshape(KB * BR, D),
        counts.reshape(KB, BR),
        block_owner.reshape(1, KB),
        block_local.reshape(1, KB),
    )
    return out.reshape(BLK, NY * NG, D)


def solution(mesh):
    finer = Mesh(mesh.devices.reshape(NX, NC, NY, NZ), ("x", "c", "y", "z"))
    return jax.shard_map(
        local,
        mesh=finer,
        in_specs=(
            P(REP, SHARD, None, None, None),
            P(REP, SHARD, None, None),
            P(REP, SHARD, None, None),
            P(REP, SHARD, None),
        ),
        out_specs=P(SHARD, REP, None),
        check_vma=False,
    )
```

```python
import math

import jax
import jax.numpy as jnp
from jax import lax
from jax.experimental import pallas as pl
from jax.experimental.pallas import tpu as pltpu
from jax.sharding import Mesh
from jax.sharding import PartitionSpec as P

NX, NC, NY, NZ = 4, 2, 4, 8
NP = NX * NC * NY
KB, BR, D = 64, 128, 128
BLK = 64
NG = BR // NP
K = NP * KB
CH = NY * BLK
PITCH = BR + 8
POS = (7, 5, 3, 1, 0, 2, 4, 6)
FIRST = 3
SUB = 2
MESH = pl.DeviceIdType.MESH
REP = ("x", "c")
SHARD = ("y", "z")
LIMIT = 0.2 * math.sqrt(BLK * NY * NZ * BR * D)


def kernel(
    grads, counts, owner, ids, out, scale,
    nat, cv, ov, iv, meta, xs, rv, mrv, kc, kt, oh, rhs, part, tpart, zr, tzr, ym, yrv, rows, nv, n1, n2s, n2,
    lsem, csem, p1s, p1r, msem, mrsem, zs, zrs, ys, yr, nsem, osem,
):
    x, c, y, z = (lax.axis_index(a) for a in ("x", "c", "y", "z"))
    me = (x * NC + c) * NY + y
    px = [lax.rem(x + d, NX) for d in range(NX)]
    pc = [c, 1 - c]
    py = [lax.rem(y + d, NY) for d in range(NY)]

    def plane(e):
        dx, dc, dy = e // (NC * NY), (e // NY) % NC, e % NY
        return {"x": px[dx], "c": pc[dc], "y": py[dy]}, (px[dx] * NC + pc[dc]) * NY + py[dy]

    def zdev(d):
        return {"z": lax.rem(z + d, NZ)}

    def wait_bytes(ref, sem):
        pltpu.make_async_copy(ref, ref, sem).wait()

    small = [
        pltpu.make_async_copy(s, d, csem.at[i])
        for i, (s, d) in enumerate(((counts, cv), (owner, ov), (ids, iv)))
    ]
    for cp in small:
        cp.start()

    def load(b, _):
        pltpu.make_async_copy(
            grads.at[pl.ds(pl.multiple_of(b * BR, 8), BR)],
            nat.at[pl.ds(pl.multiple_of(b * PITCH, 8), BR)], lsem,
        ).start()
        return 0

    lax.fori_loop(0, KB, load, 0, unroll=8)
    barrier = pltpu.get_barrier_semaphore()
    for e in range(1, NP):
        pl.semaphore_signal(barrier, inc=1, device_id=plane(e)[0], device_id_type=MESH)
    for d in range(1, NZ):
        pl.semaphore_signal(barrier, inc=1, device_id=zdev(d), device_id_type=MESH)

    for cp in small:
        cp.wait()
    o = ov[...]
    key = ((o & (NZ - 1)) * CH + (o >> 3) * BLK + iv[...]).astype(jnp.float32)
    key = jnp.broadcast_to(jnp.concatenate([key, key], axis=1), (8, 128))
    cf = cv[...].astype(jnp.float32)
    ct = jnp.concatenate([cf, cf], axis=0).T
    low = lax.broadcasted_iota(jnp.int32, (8, 128), 0) < NG
    for j in range(NP // 2):
        two = ct[8 * j : 8 * j + 8]
        meta[2 * j] = jnp.where(low, two, key)
        meta[2 * j + 1] = jnp.where(low, pltpu.roll(two, NG, 0), key)

    def prep(g):
        def one(q, _):
            xs[g, q] = nat[pl.ds(q * NG + g, KB, stride=PITCH), :]
            return 0

        lax.fori_loop(0, NP, one, 0, unroll=4)
        rv[g, me] = xs[g, me]

    def send_plane(e, src, dst, send, recv):
        dev, q = plane(e)
        pltpu.make_async_remote_copy(
            src_ref=src.at[q] if src is not nv else src, dst_ref=dst.at[me], send_sem=send, recv_sem=recv,
            device_id=dev, device_id_type=MESH,
        ).start()

    def send_p1(g):
        for i in range(NP):
            e = (i * 13 + 8 * g) % NP
            if e:
                send_plane(e, xs.at[g], rv.at[g], p1s.at[g], p1r.at[g])
            if g == 0 and i == 6:
                for f in range(1, NP):
                    send_plane(f, meta, mrv, msem, mrsem)

    def z_copy(src, dst, i, k, d, u):
        return pltpu.make_async_remote_copy(
            src_ref=src, dst_ref=dst, send_sem=zs.at[i, d, u, k], recv_sem=zrs.at[i, d, u, k],
            device_id=zdev(1 if d == 0 else NZ - 1), device_id_type=MESH,
        )

    def z_refs(p, r, k, d, u, n):
        t = 4 - k if d == 0 else 4 + k
        return p.at[POS[t % NZ], pl.ds(u * n, n)], r.at[d, u, k]

    def far(d, u, n):
        return (u * 2 * n < rows_of(n)) == (d == 0)

    def rows_of(n):
        return 16 if n == 8 else CH

    def z_step(p, r, i, j, n):
        parts = rows_of(n) // n
        for first in (True, False):
            for v in range(parts // 2):
                for d in range(2):
                    u = v if (d == 0) == first else parts // 2 + v
                    k = j if first else j + 1
                    if k > 3:
                        continue
                    own, slot = z_refs(p, r, k, d, u, n)
                    if j > 0:
                        src, dst = z_refs(p, r, k - 1, d, u, n)
                        z_copy(src, dst, i, k - 1, d, u).wait_recv()
                        own[...] += dst[...]
                    z_copy(own, slot, i, k, d, u).start()

    def z_final(p, r, i, u, n):
        for d in range(2):
            src, dst = z_refs(p, r, 3, d, u, n)
            z_copy(src, dst, i, 3, d, u).wait_recv()
        return p[POS[0], u * n : u * n + n] + r[0, u, 3] + r[1, u, 3]

    wait_bytes(nat.at[pl.ds(0, KB * BR)], lsem)
    prep(0)
    pl.semaphore_wait(barrier, NP - 1 + NZ - 1)
    send_p1(0)
    mrv[me] = meta[me]
    for g in range(1, NG):
        prep(g)
        send_p1(g)

    wait_bytes(mrv.at[pl.ds(0, NP - 1)], mrsem)

    def keys(j, _):
        lane = lax.broadcasted_iota(jnp.int32, (8, 128), 1)
        tile = jnp.where(lane < KB, mrv[2 * j], mrv[2 * j + 1])
        row = lax.broadcasted_iota(jnp.int32, (8, 128), 0)
        at = tile.astype(jnp.int32)
        t = (at >> 8) - z
        t = jnp.where(t < 0, t + NZ, t)
        t = jnp.where(t < 4, 7 - 2 * t, 2 * t - 8)
        tile = jnp.where(row < NG, tile, (t * CH + (at & (CH - 1))).astype(jnp.float32))
        kc[:, pl.ds(pl.multiple_of(j * 128, 128), 128)] = tile
        wide = jnp.concatenate([tile] * 16, axis=0)
        kt[pl.ds(pl.multiple_of(j * 128, 128), 128), :] = wide.T
        return 0

    lax.fori_loop(0, NP // 2, keys, 0, unroll=2)

    def hot(m, _):
        at = pl.multiple_of(m * 32, 32)
        rows = lax.broadcasted_iota(jnp.int32, (32, K), 0) + at
        key = jnp.broadcast_to(kc[NG : NG + 1, :].astype(jnp.int32), (32, K))
        oh[pl.ds(at, 32), :] = jnp.where(rows == key, 1.0, 0.0).astype(jnp.bfloat16)
        return 0

    lax.fori_loop(0, NZ * CH // 32, hot, 0)

    def total(t, _):
        tot = lax.dot_general(
            kc[...].astype(jnp.bfloat16), oh[pl.ds(pl.multiple_of(t * CH, CH), CH), :],
            (((1,), (1,)), ((), ())), preferred_element_type=jnp.float32,
        )
        tpart[t, 0:8] = tot[:, 0:128]
        tpart[t, 8:16] = tot[:, 128:256]
        return 0

    lax.fori_loop(0, NZ, total, 0)

    def split(g):
        wait_bytes(rv.at[g, pl.ds(0, NP - 1)], p1r.at[g])

        def one(j, _):
            at = pl.ds(pl.multiple_of(j * 128, 128), 128)
            v = rv[g, pl.ds(2 * j, 2)].reshape(128, D)
            v = jnp.where(kt[at, g : g + 1] > 0.0, v, 0.0)
            hi = v.astype(jnp.bfloat16)
            rhs[at, 0:D] = hi
            rhs[at, D : 2 * D] = (v - hi.astype(jnp.float32)).astype(jnp.bfloat16)
            return 0

        lax.fori_loop(0, NP // 2, one, 0, unroll=4)

    def combine(g, lo, n):
        both = jnp.dot(oh[lo * CH : (lo + n) * CH, :], rhs[...], preferred_element_type=jnp.float32)
        part[g, lo : lo + n] = (both[:, 0:D] + both[:, D : 2 * D]).reshape(n, CH, D)

    def finish(g):
        n = CH // SUB
        sq = jnp.zeros((8, D), jnp.float32)
        inv = [
            jnp.broadcast_to(tpart[POS[0], 8 * h + g : 8 * h + g + 1], (128, 128)).T for h in range(2)
        ]
        for v in range(SUB // 2):
            for u in (v, SUB // 2 + v):
                fin = z_final(part.at[g], zr.at[g], g, u, n)
                mean = fin * inv[u * n // 128][u * n % 128 : u * n % 128 + n]
                ym[g, u * n : u * n + n] = mean
                sq = sq + jnp.sum((mean * mean).reshape(n // 8, 8, D), axis=0)
        nv[...] = sq if g == 0 else nv[...] + sq

    def send_y(g):
        yrv[g, y] = ym[g, pl.ds(pl.multiple_of(y * BLK, BLK), BLK)]
        for dy in range(1, NY):
            pltpu.make_async_remote_copy(
                src_ref=ym.at[g, pl.ds(pl.multiple_of(py[dy] * BLK, BLK), BLK)], dst_ref=yrv.at[g, y],
                send_sem=ys.at[g], recv_sem=yr.at[g], device_id={"y": py[dy]}, device_id_type=MESH,
            ).start()

    def step(g, j):
        z_step(part.at[g], zr.at[g], g, j, CH // SUB)

    z_step(tpart, tzr, NG, 0, 8)
    for g in range(NG):
        split(g)
        combine(g, 0, FIRST)
        step(g, 0)
        if g == 0:
            z_step(tpart, tzr, NG, 1, 8)
        combine(g, FIRST, NZ - FIRST)
        if g > 0:
            step(g - 1, 3)
        step(g, 1)
        if g == 0:
            z_step(tpart, tzr, NG, 2, 8)
        if g == 1:
            for u in range(2):
                tots = z_final(tpart, tzr, NG, u, 8)
                tpart[POS[0], 8 * u : 8 * u + 8] = 1.0 / jnp.maximum(tots, 1.0)
        if g > 0:
            finish(g - 1)
            send_y(g - 1)
        step(g, 2)
        if g == 0:
            z_step(tpart, tzr, NG, 3, 8)
    step(NG - 1, 3)
    finish(NG - 1)

    for e in range(1, NP):
        send_plane(e, nv, n1, nsem.at[0], nsem.at[1])
    n1[me] = nv[...]
    send_y(NG - 1)
    wait_bytes(n1.at[pl.ds(0, NP - 1)], nsem.at[1])
    n2s[...] = jnp.sum(n1[...], axis=0)
    for d in range(1, NZ):
        pltpu.make_async_remote_copy(
            src_ref=n2s, dst_ref=n2.at[z], send_sem=nsem.at[2], recv_sem=nsem.at[3],
            device_id=zdev(d), device_id_type=MESH,
        ).start()
    n2[z] = n2s[...]
    for g in range(NG):
        wait_bytes(yrv.at[g, pl.ds(0, NY - 1)], yr.at[g])
        for s in range(NY):
            rows[pl.ds(s * NG + g, BLK, stride=NY * NG), :] = yrv[g, s]
    leave = pltpu.make_async_copy(rows, out, osem)
    leave.start()
    wait_bytes(n2.at[pl.ds(0, NZ - 1)], nsem.at[3])
    norm2 = jnp.sum(jnp.sum(n2[...], axis=0), axis=(0, 1), keepdims=True)
    scale[...] = jnp.broadcast_to(jnp.minimum(1.0, LIMIT / jnp.sqrt(norm2 + 1e-06)), (8, D))
    leave.wait()

    wait_bytes(mrv.at[pl.ds(0, NP - 1)], msem)
    for g in range(NG):
        wait_bytes(xs.at[g, pl.ds(0, NP - 1)], p1s.at[g])
        wait_bytes(yrv.at[g, pl.ds(0, NY - 1)], ys.at[g])
    for i in range(NG + 1):
        p, r, n = (tpart, tzr, 8) if i == NG else (part.at[i], zr.at[i], CH // SUB)
        for d in range(2):
            for u in range(rows_of(n) // n):
                for k in range(0 if far(d, u, n) else 1, 4):
                    z_copy(*z_refs(p, r, k, d, u, n), i, k, d, u).wait_send()
    wait_bytes(n1.at[pl.ds(0, NP - 1)], nsem.at[0])
    wait_bytes(n2.at[pl.ds(0, NZ - 1)], nsem.at[2])


def local(grads, counts, block_owner, block_local):
    f32 = jnp.float32
    i32 = jnp.int32
    vmem = pltpu.VMEM
    dma = pltpu.SemaphoreType.DMA
    mean, scale = pl.pallas_call(
        kernel,
        out_shape=(
            jax.ShapeDtypeStruct((BLK * NY * NG, D), f32),
            jax.ShapeDtypeStruct((8, D), f32),
        ),
        in_specs=[pl.BlockSpec(memory_space=pl.ANY)] * 4,
        out_specs=(pl.BlockSpec(memory_space=pl.ANY), pl.BlockSpec(memory_space=vmem)),
        scratch_shapes=[
            vmem((KB * PITCH, D), f32),
            vmem((KB, BR), i32),
            vmem((1, KB), i32),
            vmem((1, KB), i32),
            vmem((NP, 8, 128), f32),
            vmem((NG, NP, KB, D), f32),
            vmem((NG, NP, KB, D), f32),
            vmem((NP, 8, 128), f32),
            vmem((8, K), f32),
            vmem((K, 128), f32),
            vmem((NZ * CH, K), jnp.bfloat16),
            vmem((K, 2 * D), jnp.bfloat16),
            vmem((NG, NZ, CH, D), f32),
            vmem((NZ, 16, 128), f32),
            vmem((NG, 2, SUB, 4, CH // SUB, D), f32),
            vmem((2, 2, 4, 8, 128), f32),
            vmem((NG, CH, D), f32),
            vmem((NG, NY, BLK, D), f32),
            vmem((BLK * NY * NG, D), f32),
            vmem((8, D), f32),
            vmem((NP, 8, D), f32),
            vmem((8, D), f32),
            vmem((NZ, 8, D), f32),
            dma,
            dma((3,)),
            dma((NG,)),
            dma((NG,)),
            dma,
            dma,
            dma((NG + 1, 2, SUB, 4)),
            dma((NG + 1, 2, SUB, 4)),
            dma((NG,)),
            dma((NG,)),
            dma((4,)),
            dma,
        ],
        compiler_params=pltpu.CompilerParams(
            collective_id=0, has_side_effects=True, vmem_limit_bytes=52 * 2**20
        ),
        name="table_mean",
    )(
        grads.reshape(KB * BR, D),
        counts.reshape(KB, BR),
        block_owner.reshape(1, KB),
        block_local.reshape(1, KB),
    )
    return (mean.reshape(BLK, 2, 8, D) * scale).reshape(BLK, NY * NG, D)


def solution(mesh):
    finer = Mesh(mesh.devices.reshape(NX, NC, NY, NZ), ("x", "c", "y", "z"))
    return jax.shard_map(
        local,
        mesh=finer,
        in_specs=(
            P(REP, SHARD, None, None, None),
            P(REP, SHARD, None, None),
            P(REP, SHARD, None, None),
            P(REP, SHARD, None),
        ),
        out_specs=P(SHARD, REP, None),
        check_vma=False,
    )
```
